32 devices in a mesh: kpt: 2 (over y), row: 4 (over x, core), col: 4 (over z).
Axes of the slice: x: 2, y: 2, z: 4, core: 2. Of those that a mesh axis runs over, the one named last changes fastest.
Arguments:
- left_blocks: bfloat16 [8, 64, 2, 2, 128, 128], P(('kpt', 'row'), 'col'), parts along dimension 0, may hold values from -0.5 to 0.5
- left_rows: int32 [8, 64, 2], P(('kpt', 'row'), 'col'), parts along dimension 0, may hold values from 0 to 7, as said below
- left_count: int32 [8, 64], P(('kpt', 'row'), 'col'), parts along dimension 0, may hold values from 1 to 2, as said below
- left_level: int32 [8, 64, 2], P(('kpt', 'row'), 'col'), parts along dimension 0, may hold values from 0 to 7
- right_blocks: bfloat16 [2, 64, 4, 4, 2, 128, 128], P('kpt', 'row', 'col'), parts along dimension 0, may hold values from -6 to 6
- right_cols: int32 [2, 64, 4, 4], P('kpt', 'row', 'col'), parts along dimension 0, may hold values from 0 to 15, as said below
- right_count: int32 [2, 64, 4], P('kpt', 'row', 'col'), parts along dimension 0, may hold values from 1 to 4, as said below
- right_level: int32 [2, 64, 4, 4], P('kpt', 'row', 'col'), parts along dimension 0, may hold values from 0 to 7
Outputs:
- product_blocks: bfloat16 [64, 64, 2, 128, 128], P(('kpt', 'row'), 'col'), parts along dimension 0
The draws below stay inside these ranges and needn't reach their ends.
There are 2 independent parts, one for each index of `kpt`. The reference program is written for one: setup_inputs(seed, part) draws one part's arguments, and reference() takes and returns one part's arrays. A program takes and returns all parts, laid end to end along the dimension named above; each array names one. Nothing has to cross between parts.
Inputs may be any that keep to these rules, and one draw needn't show every extreme that they name: `left_rows`: the 2 slots of one row group and block column name distinct block rows. `left_count`: in every row group some block column has all 2 slots live. `right_cols`: the 4 slots of one block row and column group name distinct block columns. `right_count`: in every column group some block row has all 4 slots live.
All inputs are finite; a program needn't handle non-finite values.
Results may differ from the reference program's by a relative error of at most 0.001.
Values may be sent and summed in bfloat16 or wider, within the bound.
A program may use at most 256 MiB of HBM per device.

```python
import jax
import jax.numpy as jnp
from jax import lax

BS = 128
GR = 8
LEVEL_CUT = 7
NB = 64
KB = 16
MA = 2
MB = 4
SETS = 1
N_ROW = 4
N_COL = 4


def distinct_slots(key, count, choices, taken):
    keys = jax.random.split(key, count)
    orders = jax.vmap(lambda single: jax.random.permutation(single, choices))(keys)
    return orders[:, :taken].astype(jnp.int32)


def filled_counts(key, groups, length, most):
    base = jax.random.randint(jax.random.fold_in(key, 1), (groups, length), 1, most + 1)
    chosen = jax.random.randint(jax.random.fold_in(key, 2), (groups, 1), 0, length)
    position = jnp.arange(length, dtype=jnp.int32)[None, :]
    return jnp.where(position == chosen, most, base).astype(jnp.int32)


def draw_left_rows(key, part):
    slots = distinct_slots(jax.random.fold_in(key, 101), N_ROW * NB, GR, MA)
    return slots.reshape(N_ROW, NB, MA)


def draw_left_count(key, part):
    return filled_counts(jax.random.fold_in(key, 202), N_ROW, NB, MA)


def draw_right_cols(key, part):
    slots = distinct_slots(jax.random.fold_in(key, 303), NB * N_COL, KB, MB)
    return slots.reshape(N_COL // N_ROW, N_ROW * KB, N_COL, MB)


def draw_right_count(key, part):
    counts = filled_counts(jax.random.fold_in(key, 404), N_COL, NB, MB)
    return counts.T.reshape(N_COL // N_ROW, N_ROW * KB, N_COL)


def set_ends(array, key, low, top_value):
    longest = array.shape.index(max(array.shape))
    spots = []
    for shift in (0, 1):
        where = [jax.random.randint(jax.random.fold_in(key, axis), (), 0, length) for axis, length in enumerate(array.shape)]
        where[longest] = (where[longest] + shift) % array.shape[longest]
        spots.append(tuple(where))
    return array.at[spots[0]].set(low).at[spots[1]].set(top_value)


def shard_levels(rng, dims, cuts, least, high):
    factor_of, own = 1.0, jax.random.fold_in(rng, 6)
    for axis_at, parts in cuts:
        steps = jnp.exp(jax.random.uniform(jax.random.fold_in(own, axis_at), (parts,), jnp.float32, least / len(cuts), high / len(cuts)))
        factor_of = factor_of * jnp.repeat(steps, dims[axis_at] // parts).reshape([-1 if axis == axis_at else 1 for axis in range(len(dims))])
    return factor_of


def gaussian(rng, shape, width, limit, pieces=(), kind=jnp.bfloat16):
    values = jax.random.normal(rng, shape, jnp.float32) * width
    if len(pieces) > 0:
        values = shard_levels(rng, shape, pieces, -0.22, 0.18) * values
    return jnp.clip(values, min=-limit, max=limit).astype(kind)


def setup_inputs(seed: int = 0, part: int = 0) -> dict:
    key_list = jax.random.split(jax.random.key(seed), 9)
    own_keys = jax.random.split(jax.random.fold_in(key_list[8], part), 9)
    left_blocks = gaussian(own_keys[0], (N_ROW, NB, MA, 2, BS, BS), BS ** -0.5, 0.5, ((0, 4), (1, 4)))
    left_rows = draw_left_rows(jax.random.fold_in(jax.random.fold_in(key_list[8], part), 71), part)
    left_count = draw_left_count(jax.random.fold_in(jax.random.fold_in(key_list[8], part), 71), part)
    left_level = set_ends(jax.random.randint(own_keys[3], (N_ROW, NB, MA), 0, 8), jax.random.fold_in(own_keys[3], 1), 0, 7).astype(jnp.int32)
    right_blocks = gaussian(own_keys[4], (SETS, N_ROW * KB, N_COL, MB, 2, BS, BS), 1.0, 6.0, ((1, 4), (2, 4)))
    right_cols = draw_right_cols(jax.random.fold_in(jax.random.fold_in(key_list[8], part), 71), part)
    right_count = draw_right_count(jax.random.fold_in(jax.random.fold_in(key_list[8], part), 71), part)
    right_level = set_ends(jax.random.randint(own_keys[7], (SETS, N_ROW * KB, N_COL, MB), 0, 8), jax.random.fold_in(own_keys[7], 1), 0, 7).astype(jnp.int32)
    return dict(left_blocks=left_blocks, left_rows=left_rows, left_count=left_count, left_level=left_level, right_blocks=right_blocks, right_cols=right_cols, right_count=right_count, right_level=right_level)


def reference(left_blocks, left_rows, left_count, left_level, right_blocks, right_cols, right_count, right_level):
    right_flat = right_blocks.reshape(NB, N_COL, MB, 2, BS, BS)
    cols_flat = right_cols.reshape(NB, N_COL, MB)
    count_flat = right_count.reshape(NB, N_COL)
    level_flat = right_level.reshape(NB, N_COL, MB)
    slot_left = jnp.arange(MA, dtype=jnp.int32)
    slot_right = jnp.arange(MB, dtype=jnp.int32)
    group_base = (jnp.arange(N_ROW, dtype=jnp.int32) * GR)[:, None, None, None]
    panel_base = (jnp.arange(N_COL, dtype=jnp.int32) * KB)[None, None, :, None]

    def one_column(total, column):
        blocks_a, rows_a, count_a, level_a, blocks_b, cols_b, count_b, level_b = column
        live_a = slot_left[None, :] < count_a.astype(jnp.int32)[:, None]
        live_b = slot_right[None, :] < count_b.astype(jnp.int32)[:, None]
        kept = live_a[:, :, None, None] & live_b[None, None, :, :]
        kept = kept & (level_a.astype(jnp.int32)[:, :, None, None] + level_b.astype(jnp.int32)[None, None, :, :] >= LEVEL_CUT)
        terms = jnp.einsum("pmcij,qndjl->pmqncdil", blocks_a.astype(jnp.float32), blocks_b.astype(jnp.float32),
                           precision=lax.Precision.HIGHEST)
        real_part = terms[:, :, :, :, 0, 0] - terms[:, :, :, :, 1, 1]
        imag_part = terms[:, :, :, :, 0, 1] + terms[:, :, :, :, 1, 0]
        product = jnp.stack([real_part, imag_part], axis=4) * kept[..., None, None, None].astype(jnp.float32)
        row_index = group_base + rows_a.astype(jnp.int32)[:, :, None, None]
        col_index = panel_base + cols_b.astype(jnp.int32)[None, None, :, :]
        row_index = jnp.broadcast_to(row_index, kept.shape).reshape(-1)
        col_index = jnp.broadcast_to(col_index, kept.shape).reshape(-1)
        total = total.at[row_index, col_index].add(product.reshape(-1, 2, BS, BS))
        return total, None

    columns = (jnp.moveaxis(left_blocks, 1, 0), jnp.moveaxis(left_rows, 1, 0), jnp.moveaxis(left_count, 1, 0),
               jnp.moveaxis(left_level, 1, 0), right_flat, cols_flat, count_flat, level_flat)
    total = jnp.zeros((N_ROW * GR, NB, 2, BS, BS), jnp.float32)
    total, unused = lax.scan(one_column, total, columns)
    return total.astype(jnp.bfloat16)
```

```python
import functools

import jax
import jax.numpy as jnp
from jax import lax
from jax.experimental import pallas as pl
from jax.experimental.pallas import tpu as pltpu
from jax.sharding import PartitionSpec as P

GR = 8
LEVEL_CUT = 7
DEAD = -1000
UNROLL = 4
LEFT_CUTS = 2
RIGHT_CUTS = 4
MESH = pl.DeviceIdType.MESH


def gather_kernel(
    n_row, n_col, left, right, left_meta, right_meta,
    left_all, right_all, left_meta_all, right_meta_all,
    up_send, up_recv, down_send, down_recv,
    x_send, x_recv, own_send, own_recv, pass_send, pass_recv,
    lm_send, lm_recv, rm_send, rm_recv,
):
    row = lax.axis_index("row")
    col = lax.axis_index("col")
    n_chip = n_row // 2
    chip, core = row // 2, row % 2
    partner = chip * 2 + 1 - core

    barrier = pltpu.get_barrier_semaphore()
    for step in range(1, n_row):
        pl.semaphore_signal(
            barrier, inc=1, device_id={"row": (row + step) % n_row}, device_id_type=MESH
        )
    for step in range(1, n_col):
        pl.semaphore_signal(
            barrier, inc=1, device_id={"col": (col + step) % n_col}, device_id_type=MESH
        )
    pl.semaphore_wait(barrier, n_row + n_col - 2)

    left_size = left.shape[0] // LEFT_CUTS
    right_size = right.shape[1] // RIGHT_CUTS

    def left_copy(step, cut, up):
        panel = col - step if up else col + step
        span = pl.ds(cut * left_size, left_size)
        source = left.at[span] if step == 0 else left_all.at[panel, span]
        send, recv = (up_send, up_recv) if up else (down_send, down_recv)
        return pltpu.make_async_remote_copy(
            src_ref=source, dst_ref=left_all.at[panel, span],
            send_sem=send.at[step, cut], recv_sem=recv.at[step, cut],
            device_id={"col": col + 1 if up else col - 1}, device_id_type=MESH,
        )

    def left_sends(step, up):
        if up:
            return (col + 1 < n_col) & (col - step >= 0)
        return (col - 1 >= 0) & (col + step < n_col)

    def left_receives(step, up):
        return col - 1 - step >= 0 if up else col + 1 + step < n_col

    def across(step, cut):
        span = pl.ds(cut * right_size, right_size)
        other = ((chip + step) % n_chip) * 2 + core
        return pltpu.make_async_remote_copy(
            src_ref=right.at[:, span], dst_ref=right_all.at[:, row, span],
            send_sem=x_send.at[step - 1, cut], recv_sem=x_recv.at[step - 1, cut],
            device_id={"row": other}, device_id_type=MESH,
        )

    def passed(step, cut):
        span = pl.ds(cut * right_size, right_size)
        panel = ((chip + n_chip - step) % n_chip) * 2 + core
        return pltpu.make_async_remote_copy(
            src_ref=right_all.at[:, panel, span], dst_ref=right_all.at[:, panel, span],
            send_sem=pass_send.at[step - 1, cut], recv_sem=pass_recv.at[step - 1, cut],
            device_id={"row": partner}, device_id_type=MESH,
        )

    own = pltpu.make_async_remote_copy(
        src_ref=right, dst_ref=right_all.at[:, row],
        send_sem=own_send, recv_sem=own_recv,
        device_id={"row": partner}, device_id_type=MESH,
    )

    def meta_copies():
        for step in range(1, n_col):
            yield pltpu.make_async_remote_copy(
                src_ref=left_meta, dst_ref=left_meta_all.at[col],
                send_sem=lm_send.at[step - 1], recv_sem=lm_recv.at[step - 1],
                device_id={"col": (col + step) % n_col}, device_id_type=MESH,
            )
        for step in range(1, n_row):
            yield pltpu.make_async_remote_copy(
                src_ref=right_meta, dst_ref=right_meta_all.at[row],
                send_sem=rm_send.at[step - 1], recv_sem=rm_recv.at[step - 1],
                device_id={"row": (row + step) % n_row}, device_id_type=MESH,
            )

    for copy in meta_copies():
        copy.start()
    for cut in range(LEFT_CUTS):
        for up in (True, False):
            pl.when(left_sends(0, up))(left_copy(0, cut, up).start)
    for step in range(1, n_chip):
        for cut in range(RIGHT_CUTS):
            across(step, cut).start()
    own.start()
    left_meta_all[col] = left_meta[...]
    right_meta_all[row] = right_meta[...]

    def take_left(step, cut):
        for up in (True, False):
            pl.when(left_receives(step, up))(left_copy(step, cut, up).wait_recv)
            if step + 1 < n_col - 1:
                pl.when(left_sends(step + 1, up))(left_copy(step + 1, cut, up).start)

    def take_right(step, cut):
        across(step, cut).wait_recv()
        passed(step, cut).start()

    left_jobs = [
        ((step * LEFT_CUTS + cut + 1) / LEFT_CUTS, functools.partial(take_left, step, cut))
        for step in range(n_col - 1) for cut in range(LEFT_CUTS)
    ]
    right_jobs = [
        (2 * ((step - 1) * RIGHT_CUTS + cut + 1) / RIGHT_CUTS + 0.1,
         functools.partial(take_right, step, cut))
        for step in range(1, n_chip) for cut in range(RIGHT_CUTS)
    ]
    for _, job in sorted(left_jobs + right_jobs, key=lambda entry: entry[0]):
        job()

    own.wait()
    for step in range(1, n_chip):
        for cut in range(RIGHT_CUTS):
            across(step, cut).wait_send()
            passed(step, cut).wait()
    for step in range(n_col - 1):
        for cut in range(LEFT_CUTS):
            for up in (True, False):
                pl.when(left_sends(step, up))(left_copy(step, cut, up).wait_send)
    for copy in meta_copies():
        copy.wait()


def product_kernel(
    sizes, left, right, left_all, right_all, left_meta, right_meta,
    out, left_buf, right_buf, total, stage, pairs, counts, touched,
    left_sem, right_sem, out_sem,
):
    n_row, n_col, sets, per, ma, mb, kb_cols = sizes
    row = lax.axis_index("row")
    col = lax.axis_index("col")
    blocks = GR * kb_cols
    room = per * ma * mb + UNROLL

    def left_copy(panel, source):
        return pltpu.make_async_copy(source, left_buf.at[panel], left_sem.at[panel])

    def right_copy(panel, source):
        return pltpu.make_async_copy(source, right_buf.at[panel], right_sem.at[panel])

    for panel in range(n_col):
        which, at = panel // n_row, panel % n_row
        pl.when(col == panel)(left_copy(panel, left).start)
        pl.when(col != panel)(left_copy(panel, left_all.at[panel]).start)
        pl.when(row == at)(right_copy(panel, right.at[which]).start)
        pl.when(row != at)(right_copy(panel, right_all.at[which, at]).start)

    @pl.loop(0, blocks + 1)
    def _(block):
        touched[block] = 0

    for panel in range(n_col):
        which, at = panel // n_row, panel % n_row
        base = panel * room

        def gather(k, count):
            rights = []
            for n in range(mb):
                slot = (which * per + k) * mb + n
                rights.append((right_meta[at, 0, slot], right_meta[at, 1, slot]))
            for m in range(ma):
                slot = k * ma + m
                target = left_meta[panel, 0, slot] * kb_cols
                level = left_meta[panel, 1, slot]
                for n in range(mb):
                    code = slot * 1024 + k * mb + n
                    pairs[base + count] = code * 1024 + target + rights[n][0]
                    count = count + jnp.where(level + rights[n][1] >= LEVEL_CUT, 1, 0)
            return count

        count = lax.fori_loop(0, per, gather, jnp.int32(0))
        for extra in range(UNROLL):
            pairs[base + count + extra] = blocks
        counts[panel] = (count + UNROLL - 1) // UNROLL

    for panel in range(n_col):
        left_copy(panel, left).wait()
        right_copy(panel, right.at[0]).wait()

        @pl.loop(0, counts[panel])
        def _(group):
            done = []
            for lane in range(UNROLL):
                code = pairs[panel * room + group * UNROLL + lane]
                target = code & 1023
                block = left_buf[panel, code >> 20]
                width = block.shape[1]
                real, imag = block[:width], block[width:]
                matrix = jnp.concatenate(
                    [jnp.concatenate([real, -imag], axis=1), jnp.concatenate([imag, real], axis=1)],
                    axis=0,
                )
                other = right_buf[panel, (code >> 10) & 1023]
                done.append((target, jnp.dot(matrix, other, preferred_element_type=jnp.float32)))
            for target, product in done:
                old = touched[target] > 0
                total[target] = jnp.where(old, total[target], 0.0) + product
                touched[target] = 1

    def out_copy(line):
        span = pl.ds(line * kb_cols, kb_cols)
        return pltpu.make_async_copy(stage.at[span], out.at[span], out_sem.at[line])

    @pl.loop(0, GR)
    def _(line):
        @pl.loop(0, kb_cols, unroll=2)
        def _(k):
            block = line * kb_cols + k
            stage[block] = jnp.where(touched[block] > 0, total[block], 0.0).astype(stage.dtype)

        out_copy(line).start()

    @pl.loop(0, GR)
    def _(line):
        out_copy(line).wait()


def pack_meta(index, count, level):
    slots = index.shape[-1]
    live = jnp.arange(slots, dtype=jnp.int32) < count[..., None]
    level = jnp.where(live, level, DEAD)
    meta = jnp.stack([index.reshape(-1), level.reshape(-1)])
    width = -(-meta.shape[1] // 128) * 128
    return jnp.pad(meta, ((0, 6), (0, width - meta.shape[1])))


def body(
    n_row, n_col, left_blocks, left_rows, left_count, left_level,
    right_blocks, right_cols, right_count, right_level,
):
    _, per, ma, _, width, _ = left_blocks.shape
    sets, right_per, _, mb = right_blocks.shape[:4]
    assert right_per == per and sets * n_row == n_col and n_row % 2 == 0
    left = left_blocks.reshape(per * ma, 2 * width, width)
    right = right_blocks.reshape(sets, per * mb, 2 * width, width)
    left_meta = pack_meta(left_rows[0], left_count[0], left_level[0])
    right_meta = pack_meta(right_cols[:, :, 0], right_count[:, :, 0], right_level[:, :, 0])
    any_space = pl.BlockSpec(memory_space=pl.ANY)
    vmem = pl.BlockSpec(memory_space=pltpu.VMEM)
    smem = pl.BlockSpec(memory_space=pltpu.SMEM)
    dma = pltpu.SemaphoreType.DMA
    n_chip = n_row // 2
    left_shape = (n_col,) + left.shape
    right_shape = (sets, n_row) + right.shape[1:]
    gathered = pl.pallas_call(
        functools.partial(gather_kernel, n_row, n_col),
        out_shape=(
            jax.ShapeDtypeStruct(left_shape, left.dtype),
            jax.ShapeDtypeStruct(right_shape, right.dtype),
            jax.ShapeDtypeStruct((n_col,) + left_meta.shape, jnp.int32),
            jax.ShapeDtypeStruct((n_row,) + right_meta.shape, jnp.int32),
        ),
        in_specs=[any_space, any_space, vmem, vmem],
        out_specs=(any_space, any_space, vmem, vmem),
        scratch_shapes=[
            *[dma((n_col - 1, LEFT_CUTS))] * 4,
            *[dma((n_chip - 1, RIGHT_CUTS))] * 2,
            *[dma] * 2,
            *[dma((n_chip - 1, RIGHT_CUTS))] * 2,
            *[dma((n_col - 1,))] * 2,
            *[dma((n_row - 1,))] * 2,
        ],
        compiler_params=pltpu.CompilerParams(collective_id=0, has_side_effects=True),
        name="gather_panels",
    )(left, right, left_meta, right_meta)
    left_all, right_all, left_meta_all, right_meta_all = gathered
    kb_cols = n_row * sets * per // n_col
    blocks = GR * kb_cols
    room = per * ma * mb + UNROLL
    out = pl.pallas_call(
        functools.partial(product_kernel, (n_row, n_col, sets, per, ma, mb, kb_cols)),
        out_shape=jax.ShapeDtypeStruct((blocks, 2 * width, width), jnp.bfloat16),
        in_specs=[any_space] * 4 + [smem] * 2,
        out_specs=any_space,
        scratch_shapes=[
            pltpu.VMEM((n_col, per * ma, 2 * width, width), left.dtype),
            pltpu.VMEM((n_col, per * mb, 2 * width, width), right.dtype),
            pltpu.VMEM((blocks + 1, 2 * width, width), jnp.float32),
            pltpu.VMEM((blocks, 2 * width, width), jnp.bfloat16),
            pltpu.SMEM((n_col * room,), jnp.int32),
            pltpu.SMEM((n_col,), jnp.int32),
            pltpu.SMEM((blocks + 1,), jnp.int32),
            dma((n_col,)),
            dma((n_col,)),
            dma((GR,)),
        ],
        compiler_params=pltpu.CompilerParams(vmem_limit_bytes=60 * 1024 * 1024),
        name="pair_products",
    )(left, right, left_all, right_all, left_meta_all, right_meta_all)
    return out.reshape(GR, kb_cols, 2, width, width)


def solution(mesh):
    in_specs = (
        P(("kpt", "row"), "col", None, None, None, None),
        P(("kpt", "row"), "col", None),
        P(("kpt", "row"), "col"),
        P(("kpt", "row"), "col", None),
        P("kpt", "row", "col", None, None, None, None),
        P("kpt", "row", "col", None),
        P("kpt", "row", "col"),
        P("kpt", "row", "col", None),
    )
    out_specs = P(("kpt", "row"), "col", None, None, None)
    return jax.shard_map(
        functools.partial(body, mesh.shape["row"], mesh.shape["col"]),
        mesh=mesh, in_specs=in_specs, out_specs=out_specs, check_vma=False,
    )
```

```python
import functools

import jax
import jax.numpy as jnp
from jax import lax
from jax.experimental import pallas as pl
from jax.experimental.pallas import tpu as pltpu
from jax.sharding import PartitionSpec as P

GR = 8
LEVEL_CUT = 7
DEAD = -1000
UNROLL = 16
LEFT_CUTS = 2
VMEM_BYTES = 62 * 1024 * 1024
RIGHT_CUTS = 4
MESH = pl.DeviceIdType.MESH


def gather_kernel(
    n_row, n_col, left, right, meta,
    left_all, right_all, left_meta_all, right_meta_all,
    up_send, up_recv, down_send, down_recv,
    x_send, x_recv, own_send, own_recv, pass_send, pass_recv,
    lm_send, lm_recv, rm_send, rm_recv, left_sem, right_sem,
):
    row = lax.axis_index("row")
    col = lax.axis_index("col")
    n_chip = n_row // 2
    chip, core = row // 2, row % 2
    partner = chip * 2 + 1 - core

    barrier = pltpu.get_barrier_semaphore()
    for step in range(1, n_row):
        pl.semaphore_signal(
            barrier, inc=1, device_id={"row": (row + step) % n_row}, device_id_type=MESH
        )
    for step in range(1, n_col):
        pl.semaphore_signal(
            barrier, inc=1, device_id={"col": (col + step) % n_col}, device_id_type=MESH
        )
    pl.semaphore_wait(barrier, n_row + n_col - 2)

    left_size = left.shape[0] // LEFT_CUTS
    right_size = right.shape[1] // RIGHT_CUTS

    def left_copy(step, cut, up):
        panel = col - step if up else col + step
        span = pl.ds(cut * left_size, left_size)
        source = left.at[span] if step == 0 else left_all.at[panel, span]
        send, recv = (up_send, up_recv) if up else (down_send, down_recv)
        return pltpu.make_async_remote_copy(
            src_ref=source, dst_ref=left_all.at[panel, span],
            send_sem=send.at[step, cut], recv_sem=recv.at[step, cut],
            device_id={"col": col + 1 if up else col - 1}, device_id_type=MESH,
        )

    def left_sends(step, up):
        if up:
            return (col + 1 < n_col) & (col - step >= 0)
        return (col - 1 >= 0) & (col + step < n_col)

    def left_receives(step, up):
        return col - 1 - step >= 0 if up else col + 1 + step < n_col

    def across(step, cut):
        span = pl.ds(cut * right_size, right_size)
        other = ((chip + step) % n_chip) * 2 + core
        return pltpu.make_async_remote_copy(
            src_ref=right.at[:, span], dst_ref=right_all.at[:, row, span],
            send_sem=x_send.at[step - 1, cut], recv_sem=x_recv.at[step - 1, cut],
            device_id={"row": other}, device_id_type=MESH,
        )

    def passed(step, cut):
        span = pl.ds(cut * right_size, right_size)
        panel = ((chip + n_chip - step) % n_chip) * 2 + core
        return pltpu.make_async_remote_copy(
            src_ref=right_all.at[:, panel, span], dst_ref=right_all.at[:, panel, span],
            send_sem=pass_send.at[step - 1, cut], recv_sem=pass_recv.at[step - 1, cut],
            device_id={"row": partner}, device_id_type=MESH,
        )

    own = pltpu.make_async_remote_copy(
        src_ref=right, dst_ref=right_all.at[:, row],
        send_sem=own_send, recv_sem=own_recv,
        device_id={"row": partner}, device_id_type=MESH,
    )

    def meta_copies():
        for step in range(1, n_col):
            yield pltpu.make_async_remote_copy(
                src_ref=meta, dst_ref=left_meta_all.at[col],
                send_sem=lm_send.at[step - 1], recv_sem=lm_recv.at[step - 1],
                device_id={"col": (col + step) % n_col}, device_id_type=MESH,
            )
        for step in range(1, n_row):
            yield pltpu.make_async_remote_copy(
                src_ref=meta, dst_ref=right_meta_all.at[row],
                send_sem=rm_send.at[step - 1], recv_sem=rm_recv.at[step - 1],
                device_id={"row": (row + step) % n_row}, device_id_type=MESH,
            )

    for copy in meta_copies():
        copy.start()
    for cut in range(LEFT_CUTS):
        for up in (True, False):
            pl.when(left_sends(0, up))(left_copy(0, cut, up).start)
    for step in range(1, n_chip):
        for cut in range(RIGHT_CUTS):
            across(step, cut).start()
    own.start()
    kept = (
        pltpu.make_async_copy(left, left_all.at[col], left_sem),
        pltpu.make_async_copy(right, right_all.at[:, row], right_sem),
    )
    for copy in kept:
        copy.start()
    left_meta_all[col] = meta[...]
    right_meta_all[row] = meta[...]

    def take_left(step, cut):
        for up in (True, False):
            pl.when(left_receives(step, up))(left_copy(step, cut, up).wait_recv)
            if step + 1 < n_col - 1:
                pl.when(left_sends(step + 1, up))(left_copy(step + 1, cut, up).start)

    def take_right(step, cut):
        across(step, cut).wait_recv()
        passed(step, cut).start()

    left_jobs = [
        ((step * LEFT_CUTS + cut + 1) / LEFT_CUTS, functools.partial(take_left, step, cut))
        for step in range(n_col - 1) for cut in range(LEFT_CUTS)
    ]
    right_jobs = [
        (2 * ((step - 1) * RIGHT_CUTS + cut + 1) / RIGHT_CUTS + 0.1,
         functools.partial(take_right, step, cut))
        for step in range(1, n_chip) for cut in range(RIGHT_CUTS)
    ]
    for _, job in sorted(left_jobs + right_jobs, key=lambda entry: entry[0]):
        job()

    own.wait()
    for copy in kept:
        copy.wait()
    for step in range(1, n_chip):
        for cut in range(RIGHT_CUTS):
            across(step, cut).wait_send()
            passed(step, cut).wait()
    for step in range(n_col - 1):
        for cut in range(LEFT_CUTS):
            for up in (True, False):
                pl.when(left_sends(step, up))(left_copy(step, cut, up).wait_send)
    for copy in meta_copies():
        copy.wait()


def product_kernel(
    sizes, left, right, left_meta, right_meta, out, total, stage, pairs, touched, out_sem,
):
    n_row, n_col, sets, per, ma, mb, kb_cols = sizes
    blocks = GR * kb_cols
    tall = sets * per

    @pl.loop(0, blocks + 1)
    def _(block):
        touched[block] = 0

    count = jnp.int32(0)
    for panel in range(n_col):
        which, at = panel // n_row, panel % n_row

        def gather(k, count):
            line = which * per + k
            live = right_meta[at, tall + 1 + which, k]
            rights = []
            for n in range(mb):
                level = right_meta[at, line, 2 * ma + mb + n]
                rights.append(
                    (right_meta[at, line, 2 * ma + n], jnp.where(n < live, level, DEAD))
                )
            live = left_meta[panel, tall, k]
            slot = panel * per + k
            for m in range(ma):
                target = left_meta[panel, k, m] * kb_cols
                level = jnp.where(m < live, left_meta[panel, k, ma + m], DEAD)
                for n in range(mb):
                    code = (slot * ma + m) * 1024 + slot * mb + n
                    pairs[count] = code * 1024 + target + rights[n][0]
                    count = count + jnp.where(level + rights[n][1] >= LEVEL_CUT, 1, 0)
            return count

        count = lax.fori_loop(0, per, gather, count, unroll=4)
    for extra in range(UNROLL):
        pairs[count + extra] = blocks

    @pl.loop(0, (count + UNROLL - 1) // UNROLL)
    def _(group):
        done = []
        for lane in range(UNROLL):
            code = pairs[group * UNROLL + lane]
            target = code & 1023
            block = left[code >> 20]
            width = block.shape[1]
            real, imag = block[:width], block[width:]
            matrix = jnp.concatenate(
                [jnp.concatenate([real, -imag], axis=1), jnp.concatenate([imag, real], axis=1)],
                axis=0,
            )
            other = right[(code >> 10) & 1023]
            done.append((target, jnp.dot(matrix, other, preferred_element_type=jnp.float32)))
        for target, product in done:
            old = touched[target] > 0
            total[target] = jnp.where(old, total[target], 0.0) + product
            touched[target] = 1

    def out_copy(line):
        span = pl.ds(line * kb_cols, kb_cols)
        return pltpu.make_async_copy(stage.at[span], out.at[span], out_sem.at[line])

    @pl.loop(0, GR)
    def _(line):
        @pl.loop(0, kb_cols, unroll=4)
        def _(k):
            block = line * kb_cols + k
            stage[block] = jnp.where(touched[block] > 0, total[block], 0.0).astype(stage.dtype)

        out_copy(line).start()

    @pl.loop(0, GR)
    def _(line):
        out_copy(line).wait()


def place(array, top, lane, rows):
    tall, wide = array.shape
    return jnp.pad(array, ((top, rows - tall - top), (lane, 128 - lane - wide)))


def body(
    n_row, n_col, left_blocks, left_rows, left_count, left_level,
    right_blocks, right_cols, right_count, right_level,
):
    _, per, ma, _, width, _ = left_blocks.shape
    sets, right_per, _, mb = right_blocks.shape[:4]
    assert right_per == per and sets * n_row == n_col and n_row % 2 == 0
    left = left_blocks.reshape(per * ma, 2 * width, width)
    right = right_blocks.reshape(sets, per * mb, 2 * width, width)
    tall = sets * per
    rows = -(-(tall + 1 + sets) // 8) * 8
    meta = (
        place(jnp.concatenate([left_rows[0], left_level[0]], axis=1), 0, 0, rows)
        + place(left_count, tall, 0, rows)
        + place(
            jnp.concatenate([right_cols, right_level], axis=3).reshape(tall, 2 * mb),
            0, 2 * ma, rows,
        )
        + place(right_count.reshape(sets, per), tall + 1, 0, rows)
    )
    any_space = pl.BlockSpec(memory_space=pl.ANY)
    vmem = pl.BlockSpec(memory_space=pltpu.VMEM)
    smem = pl.BlockSpec(memory_space=pltpu.SMEM)
    dma = pltpu.SemaphoreType.DMA
    n_chip = n_row // 2
    left_shape = (n_col,) + left.shape
    right_shape = (sets, n_row) + right.shape[1:]
    limit = VMEM_BYTES - (n_col * left.size + n_row * right.size) * left.dtype.itemsize
    gathered = pl.pallas_call(
        functools.partial(gather_kernel, n_row, n_col),
        out_shape=(
            pltpu.VMEM(left_shape, left.dtype),
            pltpu.VMEM(right_shape, right.dtype),
            jax.ShapeDtypeStruct((n_col,) + meta.shape, jnp.int32),
            jax.ShapeDtypeStruct((n_row,) + meta.shape, jnp.int32),
        ),
        in_specs=[any_space, any_space, vmem],
        out_specs=(vmem, vmem, vmem, vmem),
        scratch_shapes=[
            *[dma((n_col - 1, LEFT_CUTS))] * 4,
            *[dma((n_chip - 1, RIGHT_CUTS))] * 2,
            *[dma] * 2,
            *[dma((n_chip - 1, RIGHT_CUTS))] * 2,
            *[dma((n_col - 1,))] * 2,
            *[dma((n_row - 1,))] * 2,
            *[dma] * 2,
        ],
        compiler_params=pltpu.CompilerParams(
            collective_id=0, has_side_effects=True, vmem_limit_bytes=limit
        ),
        name="gather_panels",
    )(left, right, meta)
    left_all, right_all, left_meta_all, right_meta_all = gathered
    kb_cols = n_row * sets * per // n_col
    blocks = GR * kb_cols
    out = pl.pallas_call(
        functools.partial(product_kernel, (n_row, n_col, sets, per, ma, mb, kb_cols)),
        out_shape=jax.ShapeDtypeStruct((blocks, 2 * width, width), jnp.bfloat16),
        in_specs=[vmem] * 2 + [smem] * 2,
        out_specs=any_space,
        scratch_shapes=[
            pltpu.VMEM((blocks + 1, 2 * width, width), jnp.float32),
            pltpu.VMEM((blocks, 2 * width, width), jnp.bfloat16),
            pltpu.SMEM((n_col * per * ma * mb + UNROLL,), jnp.int32),
            pltpu.SMEM((blocks + 1,), jnp.int32),
            dma((GR,)),
        ],
        compiler_params=pltpu.CompilerParams(vmem_limit_bytes=limit),
        name="pair_products",
    )(
        pltpu.with_memory_space_constraint(
            left_all.reshape((-1,) + left.shape[1:]), pltpu.VMEM
        ),
        pltpu.with_memory_space_constraint(
            right_all.reshape((-1,) + right.shape[2:]), pltpu.VMEM
        ),
        left_meta_all, right_meta_all,
    )
    return out.reshape(GR, kb_cols, 2, width, width)


def solution(mesh):
    in_specs = (
        P(("kpt", "row"), "col", None, None, None, None),
        P(("kpt", "row"), "col", None),
        P(("kpt", "row"), "col"),
        P(("kpt", "row"), "col", None),
        P("kpt", "row", "col", None, None, None, None),
        P("kpt", "row", "col", None),
        P("kpt", "row", "col"),
        P("kpt", "row", "col", None),
    )
    out_specs = P(("kpt", "row"), "col", None, None, None)
    return jax.shard_map(
        functools.partial(body, mesh.shape["row"], mesh.shape["col"]),
        mesh=mesh, in_specs=in_specs, out_specs=out_specs, check_vma=False,
    )
```
